32 devices in a mesh: groups: 2 (over y), blk: 4 (over x, core), req: 4 (over z).
Axes of the slice: x: 2, y: 2, z: 4, core: 2. Of those that a mesh axis runs over, the one named last changes fastest.
Arguments:
- hidden_states: bfloat16 [640, 4608], P(('groups', 'req'), 'blk'), parts along dimension 0, may hold values from -12 to 12
- context_lengths: int32 [128], P(('groups', 'req')), parts along dimension 0, may hold values from 64 to 512
- cache_keys: bfloat16 [128, 512, 16, 128], P(('groups', 'req'), None, 'blk'), parts along dimension 0, may hold values from -1400 to 1400
- cache_values: bfloat16 [128, 512, 16, 128], P(('groups', 'req'), None, 'blk'), parts along dimension 0, may hold values from -6 to 6
- q_weight: bfloat16 [4608, 4096], P('req', 'blk'), may hold values from -0.09375 to 0.09375
- k_weight: bfloat16 [4608, 2048], P('req', 'blk'), may hold values from -0.09375 to 0.09375
- v_weight: bfloat16 [4608, 2048], P('req', 'blk'), may hold values from -0.09375 to 0.09375
- o_weight: bfloat16 [4096, 4608], P('blk'), may hold values from -1 to 1
- gate_weight: bfloat16 [18432, 4608], P(('blk', 'req')), may hold values from -0.09375 to 0.09375
- up_weight: bfloat16 [18432, 4608], P(('blk', 'req')), may hold values from -0.09375 to 0.09375
- down_weight: bfloat16 [18432, 4608], P(('blk', 'req')), may hold values from -0.0625 to 0.0625
- attn_gain: float32 [4608], P('blk'), may hold values from 0.1 to 1.9
- post_attn_gain: float32 [4608], P('blk'), may hold values from 0.1 to 1.9
- ffn_gain: float32 [4608], P('blk'), may hold values from 0.1 to 1.9
- post_ffn_gain: float32 [4608], P('blk'), may hold values from 0.1 to 1.9
Outputs:
- layer_output: bfloat16 [640, 4608], P(('groups', 'req'), 'blk'), parts along dimension 0
- draft_keys: bfloat16 [128, 5, 16, 128], P(('groups', 'req'), None, 'blk'), parts along dimension 0
- draft_values: bfloat16 [128, 5, 16, 128], P(('groups', 'req'), None, 'blk'), parts along dimension 0
The draws below stay inside these ranges and needn't reach their ends.
There are 2 independent parts, one for each index of `groups`. The reference program is written for one: setup_inputs(seed, part) draws one part's arguments, and reference() takes and returns one part's arrays. A program takes and returns all parts, laid end to end along the dimension named above; an argument that names none is the same for every part. Nothing has to cross between parts.
All inputs are finite; a program needn't handle non-finite values.
Results may differ from the reference program's by a relative error of at most 0.015.
Values may be sent and summed in bfloat16 or wider, within the bound.
No kernel may reach another device: no remote copies, remote signals or barrier semaphores. Data moves between devices by JAX's collectives and lax.ppermute only.
A program may use at most 128 MiB of HBM per device.

```python
import math
import jax
import jax.numpy as jnp
from jax import lax

D = 4608
HEADS = 32
KV_HEADS = 16
HEAD_DIM = 128
FF = 18432
CTX = 512
DRAFT = 5
REQUESTS = 64
TOKENS = 320


def draw_hidden_states(key, part):
    keys = jax.random.split(jax.random.fold_in(key, 11), 3)
    columns = jnp.arange(D, dtype=jnp.float32) / max(D - 1, 1)
    entries = jax.random.normal(keys[0], (TOKENS, D), jnp.float32)
    row_scale = jnp.exp(jax.random.uniform(keys[1], (TOKENS, 1), jnp.float32, math.log(0.3), math.log(3.0)))
    column_scale = jnp.exp(math.log(3.0) * columns)[None, :] * jnp.exp(jax.random.uniform(keys[2], (1, D), jnp.float32, 0.0, math.log(2.0))) * 0.6
    values = entries * row_scale * column_scale
    return jnp.clip(values, -12.0, 12.0).astype(jnp.bfloat16)


def draw_cache_keys(key, part):
    keys = jax.random.split(jax.random.fold_in(key, 23), 1)
    shape = (REQUESTS, CTX, KV_HEADS, HEAD_DIM)
    values = jnp.clip(jax.random.normal(keys[0], shape, jnp.float32), -6.0, 6.0)
    return values.astype(jnp.bfloat16)


def draw_o_weight(key, part):
    keys = jax.random.split(jax.random.fold_in(key, 37), 2)
    fan_rows = HEADS * HEAD_DIM
    columns = jnp.arange(D, dtype=jnp.float32) / max(D - 1, 1)
    rough = jnp.exp(jax.random.uniform(keys[1], (1, D), jnp.float32, 0.0, math.log(2.0)))
    entries = jnp.clip(jax.random.normal(keys[0], (fan_rows, D), jnp.float32), -6.0, 6.0)
    column_scale = jnp.exp(math.log(4.0) * columns)[None, :] * rough * 0.4
    values = entries * column_scale * fan_rows ** (-0.5)
    return jnp.clip(values, -1.0, 1.0).astype(jnp.bfloat16)


def set_ends(array, stream_key, smallest, largest):
    extent = array.shape
    spot = [jax.random.randint(jax.random.fold_in(stream_key, axis), (), 0, extent[axis]) for axis in range(len(extent))]
    array = array.at[tuple(spot)].set(smallest)
    longest = extent.index(max(extent))
    spot[longest] = (spot[longest] + 1) % extent[longest]
    return array.at[tuple(spot)].set(largest)


def with_spikes(values, stream_key, source, target, blocks, factor):
    def block_of(dim):
        return (jnp.arange(values.shape[dim]) // (values.shape[dim] // blocks)).reshape((-1,) + (1,) * (values.ndim - 1 - dim))

    first = jax.random.permutation(stream_key, blocks)[block_of(target)]
    second = (block_of(target) + blocks // 2) % blocks
    return jnp.where((block_of(source) == first) | (block_of(source) == second), factor * values, values)


def level_of(own_key, extent, cuts, smallest, largest):
    level, own = 1.0, jax.random.fold_in(own_key, 6)
    for axis_at, blocks in cuts:
        heights = jnp.exp(jax.random.uniform(jax.random.fold_in(own, axis_at), (blocks,), jnp.float32, smallest / len(cuts), largest / len(cuts)))
        level = level * jnp.repeat(heights, extent[axis_at] // blocks).reshape([-1 if axis == axis_at else 1 for axis in range(len(extent))])
    return level


def scatter_about(own_key, extent, scale, bound, cuts=(), kind=jnp.bfloat16):
    values = jax.random.normal(own_key, extent, jnp.float32) * scale
    if len(cuts) > 0:
        values = level_of(own_key, extent, cuts, -0.22, 0.18) * values
    return jnp.clip(values, min=-bound, max=bound).astype(kind)


def gaussian_with(rng, extent, spread, bound, pieces, heavy, kind=jnp.bfloat16):
    values = spread * jax.random.normal(rng, extent, jnp.float32)
    if pieces:
        values = values * level_of(rng, extent, pieces, -0.22, 0.18)
    return jnp.clip(with_spikes(values, jax.random.fold_in(rng, 3), *heavy), -bound, bound).astype(kind)


def setup_inputs(seed: int = 0, part: int = 0) -> dict:
    key_list = jax.random.split(jax.random.key(seed), 16)
    part_splits = jax.random.split(jax.random.fold_in(key_list[15], part), 16)
    hidden_states = draw_hidden_states(jax.random.fold_in(jax.random.fold_in(key_list[15], part), 71), part)
    context_lengths = set_ends(jax.random.randint(part_splits[1], (REQUESTS,), CTX // 8, CTX + 1), jax.random.fold_in(part_splits[1], 1), CTX // 8, CTX).astype(jnp.int32)
    cache_keys = draw_cache_keys(jax.random.fold_in(jax.random.fold_in(key_list[15], part), 71), part)
    cache_values = scatter_about(part_splits[3], (REQUESTS, CTX, KV_HEADS, HEAD_DIM), 1.0, 6.0, ((0, 4), (2, 4)))
    q_weight = scatter_about(key_list[4], (D, HEADS * HEAD_DIM), D ** -0.5, 0.09375, ((0, 4), (1, 4)))
    k_weight = scatter_about(key_list[5], (D, KV_HEADS * HEAD_DIM), D ** -0.5, 0.09375, ((0, 4), (1, 4)))
    v_weight = scatter_about(key_list[6], (D, KV_HEADS * HEAD_DIM), D ** -0.5, 0.09375, ((0, 4), (1, 4)))
    o_weight = draw_o_weight(jax.random.fold_in(key_list[15], 71), part)
    gate_weight = scatter_about(key_list[8], (FF, D), D ** -0.5, 0.09375, ((0, 16),))
    up_weight = scatter_about(key_list[9], (FF, D), D ** -0.5, 0.09375, ((0, 16),))
    down_weight = gaussian_with(key_list[10], (FF, D), FF ** -0.5, 0.0625, ((0, 16),), (0, 1, 16, 2.0))
    attn_gain = jnp.clip(1.0 + 0.18 * jax.random.normal(key_list[11], (D,), jnp.float32), 0.1, 1.9)
    post_attn_gain = jnp.clip(1.0 + 0.18 * jax.random.normal(key_list[12], (D,), jnp.float32), 0.1, 1.9)
    ffn_gain = jnp.clip(1.0 + 0.18 * jax.random.normal(key_list[13], (D,), jnp.float32), 0.1, 1.9)
    post_ffn_gain = jnp.clip(1.0 + 0.18 * jax.random.normal(key_list[14], (D,), jnp.float32), 0.1, 1.9)
    return dict(hidden_states=hidden_states, context_lengths=context_lengths, cache_keys=cache_keys, cache_values=cache_values, q_weight=q_weight, k_weight=k_weight, v_weight=v_weight, o_weight=o_weight, gate_weight=gate_weight, up_weight=up_weight, down_weight=down_weight, attn_gain=attn_gain, post_attn_gain=post_attn_gain, ffn_gain=ffn_gain, post_ffn_gain=post_ffn_gain)


EPSILON = 1e-06
NEGATIVE = -1e+30

def rotate(values, positions):
    size = values.shape[-1]
    half = size // 2
    rates = 10000.0 ** (-(jnp.arange(half, dtype=jnp.float32) * 2.0) / size)
    angle = positions.astype(jnp.float32)[..., None] * rates
    cosine = jnp.cos(angle)
    sine = jnp.sin(angle)
    first = values[..., :half]
    second = values[..., half:]
    return jnp.concatenate([first * cosine - second * sine, second * cosine + first * sine], axis=-1)

def scaling(total):
    return lax.rsqrt(total / D + EPSILON)[:, None]

def attend_one(operands):
    queries, new_keys, new_values, old_keys, old_values, length = operands
    steps, heads, size = queries.shape
    shared = new_keys.shape[1]
    group = heads // shared
    scale = (D // HEADS) ** (-0.5)
    grouped = queries.reshape(steps, shared, group, size).astype(jnp.float32)
    older = jnp.einsum('skge,cke->kgsc', grouped, old_keys.astype(jnp.float32)) * scale
    newer = jnp.einsum('skge,tke->kgst', grouped, new_keys.astype(jnp.float32)) * scale
    valid = jnp.arange(old_keys.shape[0], dtype=jnp.int32) < length
    older = jnp.where(valid, older, NEGATIVE)
    causal = jnp.arange(steps, dtype=jnp.int32)[:, None] >= jnp.arange(steps, dtype=jnp.int32)[None, :]
    newer = jnp.where(causal, newer, NEGATIVE)
    highest = jnp.maximum(lax.optimization_barrier(jnp.max(older, axis=-1)), lax.optimization_barrier(jnp.max(newer, axis=-1)))[..., None]
    far_mass = jnp.exp(older - highest)
    near_mass = jnp.exp(newer - highest)
    total_mass = (lax.optimization_barrier(jnp.sum(far_mass, axis=-1)) + lax.optimization_barrier(jnp.sum(near_mass, axis=-1)))[..., None]
    far_weights = (far_mass / total_mass).astype(jnp.bfloat16)
    near_weights = (near_mass / total_mass).astype(jnp.bfloat16)
    blended = jnp.einsum('kgsc,cke->skge', far_weights.astype(jnp.float32), old_values.astype(jnp.float32))
    blended = blended + jnp.einsum('kgst,tke->skge', near_weights.astype(jnp.float32), new_values.astype(jnp.float32))
    return blended.reshape(steps, heads * size).astype(jnp.bfloat16)

def reference(hidden_states, context_lengths, cache_keys, cache_values, q_weight, k_weight, v_weight, o_weight, gate_weight, up_weight, down_weight, attn_gain, post_attn_gain, ffn_gain, post_ffn_gain):
    states = hidden_states.astype(jnp.float32)
    total = lax.optimization_barrier(jnp.sum(states * states, axis=1))
    normed = (states * scaling(total) * attn_gain.astype(jnp.float32)).astype(jnp.bfloat16)
    query_lin = jnp.dot(normed, q_weight, preferred_element_type=jnp.float32)
    key_lin = jnp.dot(normed, k_weight, preferred_element_type=jnp.float32)
    value_lin = jnp.dot(normed, v_weight, preferred_element_type=jnp.float32)
    positions = (context_lengths[:, None] + jnp.arange(DRAFT, dtype=jnp.int32)[None, :]).reshape(TOKENS)
    queries = rotate(query_lin.reshape(TOKENS, HEADS, HEAD_DIM), positions[:, None]).astype(jnp.bfloat16)
    new_keys = rotate(key_lin.reshape(TOKENS, KV_HEADS, HEAD_DIM), positions[:, None]).astype(jnp.bfloat16)
    draft_keys = new_keys.reshape(REQUESTS, DRAFT, KV_HEADS, HEAD_DIM)
    draft_values = value_lin.astype(jnp.bfloat16).reshape(REQUESTS, DRAFT, KV_HEADS, HEAD_DIM)
    attended = lax.map(attend_one, (queries.reshape(REQUESTS, DRAFT, HEADS, HEAD_DIM), draft_keys, draft_values, cache_keys, cache_values, context_lengths))
    attended = attended.reshape(TOKENS, HEADS * HEAD_DIM)
    mixed = jnp.dot(attended, o_weight, preferred_element_type=jnp.float32)
    total = lax.optimization_barrier(jnp.sum(mixed * mixed, axis=1))
    middle = (states + mixed * scaling(total) * post_attn_gain.astype(jnp.float32)).astype(jnp.bfloat16)
    middle_wide = middle.astype(jnp.float32)
    total = lax.optimization_barrier(jnp.sum(middle_wide * middle_wide, axis=1))
    normed_mid = (middle_wide * scaling(total) * ffn_gain.astype(jnp.float32)).astype(jnp.bfloat16)
    gate = lax.dot_general(normed_mid, gate_weight, (((1,), (1,)), ((), ())), preferred_element_type=jnp.float32)
    up = lax.dot_general(normed_mid, up_weight, (((1,), (1,)), ((), ())), preferred_element_type=jnp.float32)
    hidden = (jax.nn.gelu(gate, approximate=True) * up).astype(jnp.bfloat16)
    ffn_out = jnp.dot(hidden, down_weight, preferred_element_type=jnp.float32)
    total = lax.optimization_barrier(jnp.sum(ffn_out * ffn_out, axis=1))
    layer_output = (middle_wide + ffn_out * scaling(total) * post_ffn_gain.astype(jnp.float32)).astype(jnp.bfloat16)
    return (layer_output, draft_keys, draft_values)
```

```python
import functools

import jax
import jax.numpy as jnp
from jax import lax
from jax.experimental import pallas as pl
from jax.experimental.pallas import tpu as pltpu
from jax.sharding import PartitionSpec as P

D = 4608
HEADS = 32


EPSILON = 1e-06
NEGATIVE = -1e30
VMEM = pltpu.VMEM
GRANT = 4 << 20


def scaling(total):
    return lax.rsqrt(total / D + EPSILON)[:, None]


def angles(positions, size):
    half = size // 2
    rates = 10000.0 ** (-(jnp.arange(half, dtype=jnp.float32) * 2.0) / size)
    angle = positions.astype(jnp.float32)[:, None] * rates
    cosine = jnp.cos(angle)
    sine = jnp.sin(angle)
    return (
        jnp.concatenate([cosine, cosine], axis=1),
        jnp.concatenate([-sine, sine], axis=1),
    )


def fetch_kernel(pieces, *refs):
    count = len(refs) // 2
    sems = refs[-1]
    copies = []
    for i in range(count):
        rows = refs[i].shape[0] // pieces
        for at in range(pieces):
            part = pl.ds(at * rows, rows)
            copies.append(
                pltpu.make_async_copy(
                    refs[i].at[part], refs[count + i].at[part], sems.at[i * pieces + at]
                )
            )
    for copy in copies:
        copy.start()
    for copy in copies:
        copy.wait()


def fetch(*arrays):
    pieces = 4 if all(a.ndim == 3 or a.shape[0] % 64 == 0 for a in arrays) else 1
    size = sum(a.size * a.dtype.itemsize for a in arrays)
    return pl.pallas_call(
        functools.partial(fetch_kernel, pieces),
        out_shape=[pltpu.VMEM(a.shape, a.dtype) for a in arrays],
        in_specs=[pl.BlockSpec(memory_space=pltpu.HBM)] * len(arrays),
        out_specs=[pl.BlockSpec(memory_space=VMEM)] * len(arrays),
        scratch_shapes=[pltpu.SemaphoreType.DMA((len(arrays) * pieces,))],
        compiler_params=pltpu.CompilerParams(vmem_limit_bytes=1 << 20),
        cost_estimate=pl.CostEstimate(flops=size * 300, bytes_accessed=size, transcendentals=0),
        name="fetch",
    )(*arrays)


def add_kernel(*refs):
    total = refs[0][...].astype(jnp.float32)
    for ref in refs[1:-1]:
        total = total + ref[...].astype(jnp.float32)
    refs[-1][...] = total.astype(refs[-1].dtype)


def add_part(wholes, index, parts, rows, dtype):
    width = wholes[0].shape[1]
    if rows % 8:
        total = sum(
            [w[index * rows : (index + 1) * rows].astype(jnp.float32) for w in wholes]
            + [p.astype(jnp.float32) for p in parts]
        )
        return total.astype(dtype)
    return pl.pallas_call(
        add_kernel,
        grid=(1,),
        in_specs=[pl.BlockSpec((rows, width), lambda i: (index, 0))] * len(wholes)
        + [pl.BlockSpec((rows, width), lambda i: (0, 0))] * len(parts),
        out_specs=pl.BlockSpec((rows, width), lambda i: (0, 0)),
        out_shape=jax.ShapeDtypeStruct((rows, width), dtype),
        compiler_params=pltpu.CompilerParams(vmem_limit_bytes=8 << 20),
        name="add_part",
    )(*wholes, *parts)


def project_kernel(parts, own_ref, x_ref, q_ref, k_ref, v_ref, *rest):
    outs, scaled = rest[:parts], rest[parts]
    rows = x_ref.shape[0] // parts
    for part in range(parts):
        source = lax.rem(own_ref[0] + part, parts)
        scaled[part * rows : (part + 1) * rows, :] = x_ref[
            pl.ds(pl.multiple_of(source * rows, 8), rows), :
        ]
    start = 0
    for weight in (q_ref, k_ref, v_ref):
        width = weight.shape[1]
        product = jnp.dot(scaled[...], weight[...], preferred_element_type=jnp.float32)
        for part in range(parts):
            outs[part][:, start : start + width] = product[
                part * rows : (part + 1) * rows
            ].astype(jnp.bfloat16)
        start += width


def project(own, x, q_weight, k_weight, v_weight, parts):
    rows = x.shape[0] // parts
    width = q_weight.shape[1] + k_weight.shape[1] + v_weight.shape[1]
    spec = pl.BlockSpec(memory_space=VMEM)
    return pl.pallas_call(
        functools.partial(project_kernel, parts),
        out_shape=[jax.ShapeDtypeStruct((rows, width), jnp.bfloat16)] * parts,
        in_specs=[pl.BlockSpec(memory_space=pltpu.SMEM)] + [spec] * 4,
        out_specs=[spec] * parts,
        scratch_shapes=[VMEM(x.shape, jnp.bfloat16)],
        compiler_params=pltpu.CompilerParams(vmem_limit_bytes=24 << 20),
        cost_estimate=pl.CostEstimate(
            flops=2 * x.shape[0] * x.shape[1] * width,
            bytes_accessed=2 * x.shape[1] * width,
            transcendentals=0,
        ),
        name="project",
    )(own, x, q_weight, k_weight, v_weight)


def attend_kernel(parts, req_count, kv_count, scale, *refs):
    lengths = refs[0]
    pieces = refs[1 : 1 + parts]
    (row_scale, cosine, sine, keys, values, attended, new_keys, new_values) = refs[
        1 + parts : 9 + parts
    ]
    flat, lin, mixed, packed, code = refs[9 + parts :]
    step = pl.program_id(0)
    rows, width = pieces[0].shape
    steps = rows // req_count
    size = keys.shape[-1]
    kv_width = kv_count * size
    q_width = width - 2 * kv_width
    heads = q_width // size
    group = heads // kv_count
    slots = keys.shape[1]
    shift = kv_count.bit_length() - 1

    @pl.when(step == 0)
    def _():
        total = pieces[0][...].astype(jnp.float32)
        for piece in pieces[1:]:
            total = total + piece[...].astype(jnp.float32)
        total = total * row_scale[...]
        for at in range((q_width + kv_width) // size):
            lanes = slice(at * size, (at + 1) * size)
            vector = total[:, lanes]
            turned = (
                vector * cosine[...] + pltpu.roll(vector, size // 2, 1) * sine[...]
            ).astype(jnp.bfloat16)
            flat[:rows, lanes] = turned.astype(jnp.float32)
            if at >= heads:
                new_keys[:, (at - heads) * size : (at - heads + 1) * size] = turned
        plain = total[:, q_width + kv_width :].astype(jnp.bfloat16)
        new_values[...] = plain
        flat[:rows, q_width + kv_width :] = plain.astype(jnp.float32)
        flat[rows:, :] = jnp.zeros((flat.shape[0] - rows, width), jnp.float32)
        for at in range(req_count):
            lin[at * 8 : (at + 1) * 8, :] = flat[at * steps : at * steps + 8, :]
        row = lax.broadcasted_iota(jnp.int32, code.shape, 0)
        column = lax.broadcasted_iota(jnp.int32, code.shape, 1)
        owner = jnp.right_shift(row, 3)
        shared = jnp.zeros_like(owner)
        for head in range(heads):
            shared = jnp.where(owner == head, head // group, shared)
        code[...] = jnp.where(
            jnp.bitwise_and(column, kv_count - 1) == shared,
            jnp.right_shift(column, shift),
            jnp.int32(1 << 30),
        )

    base = q_width + kv_width
    dims = (((1,), (1,)), ((), ()))
    factor = scale * 1.4426950408889634
    row = lax.broadcasted_iota(jnp.int32, (heads * 8, kv_count * 8), 0)
    column = lax.broadcasted_iota(jnp.int32, (heads * 8, kv_count * 8), 1)
    owner = jnp.right_shift(row, 3)
    shared = jnp.zeros_like(owner)
    for head in range(heads):
        shared = jnp.where(owner == head, head // group, shared)
    draft = jnp.bitwise_and(column, 7)
    allowed = (
        (jnp.right_shift(column, 3) == shared)
        & (draft <= jnp.bitwise_and(row, 7))
        & (draft < steps)
    )

    def one(request, taken):
        first = pl.multiple_of(request * 8, 8)
        now = lin[pl.ds(first, 8), :]

        def stacked(start, count):
            return jnp.concatenate(
                [now[:, start + i * size : start + (i + 1) * size] for i in range(count)], axis=0
            ).astype(jnp.bfloat16)

        query = stacked(0, heads)
        older = lax.dot_general(
            query, keys[request, :taken], dims, preferred_element_type=jnp.float32
        )
        older = jnp.where(code[:, :taken] < lengths[request], older, NEGATIVE)
        newer = lax.dot_general(
            query, stacked(q_width, kv_count), dims, preferred_element_type=jnp.float32
        )
        newer = jnp.where(allowed, newer, NEGATIVE)
        highest = jnp.maximum(
            jnp.max(older, axis=1, keepdims=True), jnp.max(newer, axis=1, keepdims=True)
        )
        far = jnp.exp2((older - highest) * factor)
        near = jnp.exp2((newer - highest) * factor)
        mass = jnp.sum(far, axis=1, keepdims=True) + jnp.sum(near, axis=1, keepdims=True)
        blended = jnp.dot(
            far.astype(jnp.bfloat16), values[request, :taken], preferred_element_type=jnp.float32
        )
        blended = blended + jnp.dot(
            near.astype(jnp.bfloat16), stacked(base, kv_count), preferred_element_type=jnp.float32
        )
        blended = blended / mass
        for h in range(heads):
            mixed[pl.ds(first, 8), h * size : (h + 1) * size] = blended[h * 8 : (h + 1) * 8]

    together = 2 if req_count % 2 == 0 else 1
    needed = lengths[step * together]
    for i in range(1, together):
        needed = jnp.maximum(needed, lengths[step * together + i])
    chunks = 4 if (slots // kv_count) % 4 == 0 else 1
    span = slots // kv_count // chunks
    for chunk in range(chunks):
        fits = needed > chunk * span
        if chunk < chunks - 1:
            fits = fits & (needed <= (chunk + 1) * span)

        @pl.when(fits)
        def _(chunk=chunk):
            for i in range(together):
                one(step * together + i, (chunk + 1) * span * kv_count)

    @pl.when(step == req_count // together - 1)
    def _():
        for at in range(req_count):
            packed[at * steps : (at + 1) * steps, :] = mixed[at * 8 : at * 8 + steps, :]
        attended[...] = packed[...].astype(jnp.bfloat16)


def attend(lengths, pieces, row_scale, cosine, sine, keys, values, kv_count):
    rows, width = pieces[0].shape
    req_count, slots, size = keys.shape
    kv_width = kv_count * size
    heads = (width - 2 * kv_width) // size
    spec = pl.BlockSpec(memory_space=VMEM)
    whole = lambda shape: pl.BlockSpec(shape, lambda i, n: (0,) * len(shape))
    return pl.pallas_call(
        functools.partial(
            attend_kernel, len(pieces), req_count, kv_count, (D // HEADS) ** (-0.5)
        ),
        grid_spec=pltpu.PrefetchScalarGridSpec(
            num_scalar_prefetch=1,
            grid=(req_count // 2 if req_count % 2 == 0 else req_count,),
            in_specs=[whole(p.shape) for p in pieces]
            + [
                whole(row_scale.shape),
                whole(cosine.shape),
                whole(sine.shape),
                spec,
                spec,
            ],
            out_specs=[
                whole((rows, heads * size)),
                whole((rows, kv_width)),
                whole((rows, kv_width)),
            ],
            scratch_shapes=[
                VMEM((rows + 8, width), jnp.float32),
                VMEM((req_count * 8, width), jnp.float32),
                VMEM((req_count * 8, heads * size), jnp.float32),
                VMEM((rows, heads * size), jnp.float32),
                VMEM((heads * 8, slots), jnp.int32),
            ],
        ),
        out_shape=[
            jax.ShapeDtypeStruct((rows, heads * size), jnp.bfloat16),
            jax.ShapeDtypeStruct((rows, kv_width), jnp.bfloat16),
            jax.ShapeDtypeStruct((rows, kv_width), jnp.bfloat16),
        ],
        compiler_params=pltpu.CompilerParams(vmem_limit_bytes=6 << 20),
        cost_estimate=pl.CostEstimate(
            flops=4 * req_count * heads * 8 * slots * size,
            bytes_accessed=4 * req_count * slots * size,
            transcendentals=req_count * heads * 8 * slots,
        ),
        name="attend",
    )(lengths, *pieces, row_scale, cosine, sine, keys, values)


def half_kernel(block, half_ref, a_ref, w_ref, out_ref):
    width = out_ref.shape[1]
    first = half_ref[0] * width
    if len(a_ref.shape) == 2:
        a = a_ref[...]
    else:
        a = jnp.concatenate([a_ref[i] for i in range(a_ref.shape[0])], axis=1)
    for at in range(width // block):
        lanes = pl.ds(pl.multiple_of(first + at * block, 128), block)
        out_ref[:, at * block : (at + 1) * block] = jnp.dot(
            a, w_ref[:, lanes], preferred_element_type=jnp.float32
        ).astype(out_ref.dtype)


def half_product(half, a, weight, dtype):
    rows, depth = a.shape[-2], weight.shape[0]
    width = weight.shape[1] // 2
    block = 256 if width % 256 == 0 else 128
    spec = pl.BlockSpec(memory_space=VMEM)
    return pl.pallas_call(
        functools.partial(half_kernel, block),
        in_specs=[pl.BlockSpec(memory_space=pltpu.SMEM), spec, spec],
        out_specs=spec,
        out_shape=jax.ShapeDtypeStruct((rows, width), dtype),
        compiler_params=pltpu.CompilerParams(vmem_limit_bytes=GRANT),
        cost_estimate=pl.CostEstimate(
            flops=2 * rows * depth * width,
            bytes_accessed=2 * depth * width,
            transcendentals=0,
        ),
        name="half_product",
    )(half, a, weight)


def hidden_kernel(block, core_ref, own_ref, other_ref, gate_ref, up_ref, out_ref):
    width = own_ref.shape[1]
    units = gate_ref.shape[0]
    core = core_ref[0]
    dims = (((1,), (1,)), ((), ()))

    def step(at, carry):
        rows = pl.ds(pl.multiple_of(at * block, 8), block)

        def columns(half):
            lanes = pl.ds(pl.multiple_of(half * width, 128), width)
            return jnp.concatenate([gate_ref[rows, lanes], up_ref[rows, lanes]], axis=0)

        both = lax.dot_general(
            own_ref[...], columns(core), dims, preferred_element_type=jnp.float32
        ) + lax.dot_general(
            other_ref[...], columns(1 - core), dims, preferred_element_type=jnp.float32
        )
        out_ref[at] = (
            jax.nn.gelu(both[:, :block], approximate=True) * both[:, block:]
        ).astype(jnp.bfloat16)
        return carry

    lax.fori_loop(0, units // block, step, 0)


def hidden_units(core, own, other, gate_weight, up_weight):
    rows, width = own.shape
    units, depth = gate_weight.shape
    block = 128 if units % 128 == 0 else units
    count = units // block
    spec = pl.BlockSpec(memory_space=VMEM)
    return pl.pallas_call(
        functools.partial(hidden_kernel, block),
        in_specs=[pl.BlockSpec(memory_space=pltpu.SMEM), spec, spec, spec, spec],
        out_specs=spec,
        out_shape=jax.ShapeDtypeStruct((count, rows, block), jnp.bfloat16),
        compiler_params=pltpu.CompilerParams(vmem_limit_bytes=GRANT),
        cost_estimate=pl.CostEstimate(
            flops=4 * rows * depth * units,
            bytes_accessed=4 * depth * units,
            transcendentals=rows * units,
        ),
        name="hidden_units",
    )(core, own, other, gate_weight, up_weight)


def body(
    hidden_states,
    context_lengths,
    cache_keys,
    cache_values,
    q_weight,
    k_weight,
    v_weight,
    o_weight,
    gate_weight,
    up_weight,
    down_weight,
    attn_gain,
    post_attn_gain,
    ffn_gain,
    post_ffn_gain,
):
    blk, req = lax.axis_size("blk"), lax.axis_size("req")
    pairs = blk // 2
    b, r = lax.axis_index("blk"), lax.axis_index("req")
    x, core = b // 2, b % 2
    core_at = core[None].astype(jnp.int32)
    token_rows, features = hidden_states.shape
    req_count = context_lengths.shape[0]
    steps = token_rows // req_count
    _, slots, kv_count, size = cache_keys.shape
    part = token_rows // pairs

    def along_blk(value, to):
        return lax.ppermute(value, "blk", [(i, to(i)) for i in range(blk)])

    def to_core(value):
        return along_blk(value, lambda i: i ^ 1)

    def to_pair(value, hop):
        return along_blk(value, lambda i: (i // 2 + hop) % pairs * 2 + i % 2)

    def to_request(value, hop):
        return lax.ppermute(value, "req", [(i, (i + hop) % req) for i in range(req)])

    def own_rows(value, index):
        return lax.dynamic_slice_in_dim(value, index * part, part, 0)

    weights = fetch(q_weight, k_weight, v_weight)
    raised = (hidden_states.astype(jnp.float32) * attn_gain).astype(jnp.bfloat16)
    if blk == req and features == q_weight.shape[0]:
        turn = [(i * req + j, j * blk + i) for i in range(blk) for j in range(req)]
        moved = lax.ppermute(raised, ("blk", "req"), turn)
        gathered = lax.all_gather(moved, "blk", axis=0, tiled=True)
    else:
        rows = lax.all_gather(raised, "blk", axis=1, tiled=True)
        gathered = lax.all_to_all(rows, "req", split_axis=1, concat_axis=0, tiled=True)

    partial = project(r[None].astype(jnp.int32), gathered, *weights, req)
    hidden_states, post_attn_gain, partial = lax.optimization_barrier(
        (hidden_states, post_attn_gain, partial)
    )
    hops = sorted(range(1, req), key=lambda hop: -min(hop, req - hop))
    pieces = [partial[0]] + [to_request(partial[hop], hop) for hop in hops]

    states = hidden_states.astype(jnp.float32)
    local = jnp.sum(states * states, axis=1)
    if blk <= 4:
        total = local
        for hop in range(1, blk):
            total = total + along_blk(local, lambda i, hop=hop: (i + hop) % blk)
    else:
        total = lax.psum(local, "blk")
    total, cache_keys, cache_values, o_weight, gate_weight = lax.optimization_barrier(
        (total, cache_keys, cache_values, o_weight, gate_weight)
    )
    cache_keys, cache_values = fetch(
        cache_keys.reshape(req_count, slots * kv_count, size),
        cache_values.reshape(req_count, slots * kv_count, size),
    )
    (o_weight,) = fetch(o_weight)
    (gate_weight,) = fetch(gate_weight)
    gains = jnp.stack([post_attn_gain, ffn_gain, post_ffn_gain])
    held, held_gains = [], []
    for hop in range(pairs):
        to = lambda i, hop=hop: (i % pairs + hop) % pairs * 2 + i // pairs
        held.append(along_blk(own_rows(hidden_states, (b % pairs + hop) % pairs), to))
        held_gains.append(along_blk(gains, to))

    def in_order(list_of, axis):
        stacked = jnp.stack(list_of)
        return jnp.concatenate(
            [
                lax.dynamic_index_in_dim(stacked, (x + pairs - m) % pairs, 0, keepdims=False)
                for m in range(pairs)
            ],
            axis=axis,
        )

    residual = in_order(held, 1).astype(jnp.float32)
    post_attn_half, ffn_half, post_ffn_half = in_order(held_gains, 1)

    positions = (context_lengths[:, None] + jnp.arange(steps, dtype=jnp.int32)[None, :]).reshape(
        token_rows
    )
    cosine, sine = angles(positions, size)
    attended, new_keys, new_values = attend(
        context_lengths,
        pieces,
        scaling(total),
        cosine,
        sine,
        cache_keys,
        cache_values,
        kv_count,
    )
    draft_keys = new_keys.reshape(req_count, steps, kv_count, size)
    draft_values = new_values.reshape(req_count, steps, kv_count, size)

    passed = half_product(1 - core_at, attended, o_weight, jnp.bfloat16)
    passed = to_core(passed)
    kept = half_product(core_at, attended, o_weight, jnp.float32)
    both = kept + passed.astype(jnp.float32)
    mixed = own_rows(both, x)
    for hop in range(1, pairs):
        mixed = mixed + to_pair(
            own_rows(both, (x + hop) % pairs).astype(jnp.bfloat16), hop
        ).astype(jnp.float32)

    def row_total(value):
        own = jnp.sum(value * value, axis=1)
        return own + to_core(own)

    middle = (residual + mixed * scaling(row_total(mixed)) * post_attn_half).astype(jnp.bfloat16)
    middle_wide = middle.astype(jnp.float32)
    normed = (middle_wide * scaling(row_total(middle_wide)) * ffn_half).astype(jnp.bfloat16)

    normed, up_weight, down_weight = lax.optimization_barrier((normed, up_weight, down_weight))
    (up_weight,) = fetch(up_weight)
    (down_weight,) = fetch(down_weight)
    order = [0] + hops
    column = [normed] + [to_request(normed, hop) for hop in hops]
    columns = [column] + [
        [to_pair(block, hop) for block in column] for hop in range(1, pairs)
    ]
    hidden = []
    for blocks in columns:
        own = jnp.concatenate(blocks, axis=0)
        hidden.append(hidden_units(core_at, own, to_core(own), gate_weight, up_weight))

    back = []
    for hop in list(range(1, pairs)) + [0]:
        passed = to_core(half_product(1 - core_at, hidden[hop], down_weight, jnp.bfloat16))
        kept = half_product(core_at, hidden[hop], down_weight, jnp.float32)
        if hop:
            back.append(
                {
                    k: to_pair(
                        add_part([kept, passed], order.index(k), [], part, jnp.bfloat16),
                        pairs - hop,
                    )
                    for k in hops + [0]
                }
            )
    returned = [
        to_request(
            add_part([kept, passed], order.index(k), [b[k] for b in back], part, jnp.bfloat16),
            req - k,
        )
        for k in hops
    ]
    ffn_out = add_part([kept, passed], 0, [b[0] for b in back] + returned, part, jnp.float32)
    result = (middle_wide + ffn_out * scaling(row_total(ffn_out)) * post_ffn_half).astype(
        jnp.bfloat16
    )

    received = []
    for hop in range(pairs):
        to = lambda i, hop=hop: i % 2 * pairs + (i // 2 + hop) % pairs
        columns = lax.dynamic_slice_in_dim(result, (x + hop) % pairs * features, features, 1)
        received.append(along_blk(columns, to))
    stacked = jnp.stack(received)
    m = b % pairs
    layer_output = jnp.concatenate(
        [
            lax.dynamic_index_in_dim(stacked, (m + pairs - at) % pairs, 0, keepdims=False)
            for at in range(pairs)
        ],
        axis=0,
    )
    return (layer_output, draft_keys, draft_values)


def solution(mesh):
    placed = (
        P(("groups", "req"), "blk"),
        P(("groups", "req")),
        P(("groups", "req"), None, "blk", None),
        P(("groups", "req"), None, "blk", None),
        P("req", "blk"),
        P("req", "blk"),
        P("req", "blk"),
        P("blk", None),
        P(("blk", "req"), None),
        P(("blk", "req"), None),
        P(("blk", "req"), None),
        P("blk"),
        P("blk"),
        P("blk"),
        P("blk"),
    )
    return jax.shard_map(
        body,
        mesh=mesh,
        in_specs=placed,
        out_specs=(
            P(("groups", "req"), "blk"),
            P(("groups", "req"), None, "blk", None),
            P(("groups", "req"), None, "blk", None),
        ),
        check_vma=False,
    )
```
